512 devices in a mesh: fsdp: 32 (over y, x, core), seq: 16 (over z).
Axes of the slice: x: 4, y: 4, z: 16, core: 2. Of those that a mesh axis runs over, the one named last changes fastest.
Arguments:
- query_rows: bfloat16 [64, 3072, 16, 128], P('fsdp', 'seq'), may hold values from -6 to 6
- key_rows: bfloat16 [64, 3072, 16, 128], P('fsdp', 'seq'), may hold values from -6 to 6
- value_rows: bfloat16 [64, 3072, 16, 128], P('fsdp', 'seq'), may hold values from -6 to 6
- gate_rows: bfloat16 [64, 3072, 16, 128], P('fsdp', 'seq'), may hold values from -6 to 6
- out_weight: bfloat16 [2048, 2048], P('fsdp'), may hold values from -0.125 to 0.125
Outputs:
- block_out: bfloat16 [64, 3072, 2048], P('fsdp', 'seq')
The draws below stay inside these ranges and needn't reach their ends.
All inputs are finite; a program needn't handle non-finite values.
Results may differ from the reference program's by a relative error of at most 0.006.
Values may be sent and summed in bfloat16 or wider, within the bound.
No kernel may reach another device: no remote copies, remote signals or barrier semaphores. Data moves between devices by JAX's collectives and lax.ppermute only.
A program may use at most 64 MiB of HBM per device.

```python
import jax
import jax.numpy as jnp
from jax import lax

HEADS = 16
HEAD_SIZE = 128
BATCH = 64
TOKENS = 3072
WIDTH = 2048


def block_scale(own_key, dims, shards, low, top_value):
    loudness, own = 1.0, jax.random.fold_in(own_key, 6)
    for axis_at, blocks in shards:
        steps = jnp.exp(jax.random.uniform(jax.random.fold_in(own, axis_at), (blocks,), jnp.float32, low / len(shards), top_value / len(shards)))
        loudness = loudness * jnp.repeat(steps, dims[axis_at] // blocks).reshape([-1 if axis == axis_at else 1 for axis in range(len(dims))])
    return loudness


def gaussian(rng, extent, deviation, reach, split=(), dtype=jnp.bfloat16):
    drawn = jax.random.normal(rng, extent, jnp.float32) * deviation
    if len(split) > 0:
        drawn = block_scale(rng, extent, split, -0.22, 0.18) * drawn
    return jnp.clip(drawn, min=-reach, max=reach).astype(dtype)


def setup_inputs(seed: int = 0) -> dict:
    keys = jax.random.split(jax.random.key(seed), 6)
    query_rows = gaussian(keys[0], (BATCH, TOKENS, HEADS, HEAD_SIZE), 1.0, 6.0, ((0, 32), (1, 16)))
    key_rows = gaussian(keys[1], (BATCH, TOKENS, HEADS, HEAD_SIZE), 1.0, 6.0, ((0, 32), (1, 16)))
    value_rows = gaussian(keys[2], (BATCH, TOKENS, HEADS, HEAD_SIZE), 1.0, 6.0, ((0, 32), (1, 16)))
    gate_rows = gaussian(keys[3], (BATCH, TOKENS, HEADS, HEAD_SIZE), 1.0, 6.0, ((0, 32), (1, 16)))
    out_weight = gaussian(keys[4], (WIDTH, WIDTH), WIDTH ** -0.5, 0.125, ((0, 32),))
    return dict(query_rows=query_rows, key_rows=key_rows, value_rows=value_rows, gate_rows=gate_rows, out_weight=out_weight)


def feature_map(values):
    wide = values.astype(jnp.float32)
    return (wide * wide + 0.1).astype(jnp.bfloat16)


def finish_heads(read, gate_rows, count):
    result = read * count ** 0.5
    result = result * jax.nn.sigmoid(gate_rows.astype(jnp.float32))
    return result.astype(jnp.bfloat16)


def read_state(features, state, mass):
    small = lax.optimization_barrier(state.astype(jnp.bfloat16))
    top = jnp.einsum("bthd,bhde->bthe", features.astype(jnp.float32), small.astype(jnp.float32))
    bottom = jnp.einsum("bthd,bhd->bth", features.astype(jnp.float32), mass, precision=lax.Precision.HIGHEST)
    return top / (bottom + 1e-3)[..., None]


def reference(query_rows, key_rows, value_rows, gate_rows, out_weight):
    query_feature, key_feature = lax.optimization_barrier((feature_map(query_rows), feature_map(key_rows)))
    state = jnp.einsum("bthd,bthe->bhde", key_feature.astype(jnp.float32), value_rows.astype(jnp.float32)) / TOKENS
    mass = jnp.sum(key_feature.astype(jnp.float32), axis=1) / TOKENS
    mixed = finish_heads(read_state(query_feature, state, mass), gate_rows, TOKENS).reshape(BATCH, TOKENS, WIDTH)
    mixed = lax.optimization_barrier(mixed)
    block_out = jnp.einsum("btw,wv->btv", mixed.astype(jnp.float32), out_weight.astype(jnp.float32)).astype(jnp.bfloat16)
    return block_out
```

```python
import jax
import jax.numpy as jnp
from jax import lax
from jax.sharding import Mesh, PartitionSpec as P


def feature_map(values):
    wide = values.astype(jnp.float32)
    return (wide * wide + 0.1).astype(jnp.bfloat16)


def finish_heads(read, gate_rows, count):
    result = read * count**0.5
    result = result * jax.nn.sigmoid(gate_rows.astype(jnp.float32))
    return result.astype(jnp.bfloat16)


def read_state(features, state, mass):
    top = jnp.einsum(
        "bthd,bhde->bthe", features, state.astype(jnp.bfloat16), preferred_element_type=jnp.float32
    )
    bottom = jnp.einsum("bthd,bhd->bth", features.astype(jnp.float32), mass)
    return top / (bottom + 0.001)[..., None]


def sum_over_seq(part_state, part_mass):
    pairs = part_state.reshape(64, 64, 128)
    summed = lax.psum([pairs[i] for i in range(64)] + [part_mass.reshape(32, 128)], "z")
    state = jnp.stack(summed[:64]).reshape(part_state.shape)
    return state, summed[64].reshape(part_mass.shape)


def local(query_rows, key_rows, value_rows, gate_rows, out_weight):
    copies = jnp.broadcast_to(out_weight[None], (16, *out_weight.shape))
    own = lax.all_to_all(copies, ("y", "x"), 0, 0, tiled=True)
    query_feature, key_feature = (feature_map(query_rows), feature_map(key_rows))
    count = query_rows.shape[1] * lax.axis_size("z")
    part_state = jnp.einsum(
        "bthd,bthe->bhde", key_feature, value_rows, preferred_element_type=jnp.float32
    )
    part_mass = jnp.sum(key_feature.astype(jnp.float32), axis=1)
    state, mass = sum_over_seq(
        (part_state / count).astype(jnp.bfloat16), (part_mass / count).astype(jnp.bfloat16)
    )
    other = lax.ppermute(own, "c", [(0, 1), (1, 0)])
    read = read_state(query_feature, state, mass.astype(jnp.float32))
    mixed = finish_heads(read, gate_rows, count)
    mixed = mixed.reshape(mixed.shape[0], mixed.shape[1], -1)
    first = lax.axis_index("c") == 0
    weight = jnp.stack([jnp.where(first, own, other), jnp.where(first, other, own)], axis=1)
    return jnp.einsum(
        "btw,wv->btv",
        mixed,
        weight.reshape(-1, weight.shape[-1]),
        preferred_element_type=jnp.float32,
    ).astype(jnp.bfloat16)


def solution(mesh):
    grid = Mesh(mesh.devices.reshape(4, 4, 2, 16), ("y", "x", "c", "z"))
    rows = P(("y", "x", "c"), "z", None, None)
    in_specs = (rows, rows, rows, rows, P(("y", "x", "c"), None))
    out_specs = P(("y", "x", "c"), "z", None)
    return jax.shard_map(local, mesh=grid, in_specs=in_specs, out_specs=out_specs, check_vma=False)
```

```python
import functools

import jax
import jax.numpy as jnp
from jax import lax
from jax.experimental import pallas as pl
from jax.experimental.pallas import tpu as pltpu
from jax.sharding import Mesh, PartitionSpec as P

PIECES = 64
COLUMNS = 512


def vmem():
    return pl.BlockSpec(memory_space=pltpu.VMEM)


def room(mib):
    return pltpu.CompilerParams(vmem_limit_bytes=mib * 2**20)


def feature_map(values):
    wide = values.astype(jnp.float32)
    return (wide * wide + 0.1).astype(jnp.bfloat16)


def finish_heads(read, gate_rows, count):
    result = read * count**0.5
    gates = jnp.swapaxes(gate_rows, 1, 2).astype(jnp.float32)
    result = result * jax.nn.sigmoid(gates)
    return result.astype(jnp.bfloat16)


def read_state(features, state, mass):
    top = jnp.einsum(
        "bthd,bhde->bhte", features, state.astype(jnp.bfloat16), preferred_element_type=jnp.float32
    )
    bottom = jnp.einsum("bthd,bhd->bht", features.astype(jnp.float32), mass)
    return top / (bottom + 0.001)[..., None]


def copies_kernel(weight_ref, out_ref, sems):
    moves = [
        pltpu.make_async_copy(weight_ref, out_ref.at[i], sems.at[i])
        for i in range(out_ref.shape[0])
    ]
    for move in moves:
        move.start()
    for move in moves:
        move.wait()


def copies_of(weight, number):
    return pl.pallas_call(
        copies_kernel,
        out_shape=jax.ShapeDtypeStruct((number, *weight.shape), weight.dtype),
        in_specs=[vmem()],
        out_specs=pl.BlockSpec(memory_space=pl.ANY),
        scratch_shapes=[pltpu.SemaphoreType.DMA((number,))],
        compiler_params=room(2),
        name="copies",
    )(weight)


def split_kernel(state_ref, mass_ref, *out_refs):
    for i in range(PIECES):
        out_refs[i][...] = state_ref[i].astype(jnp.bfloat16)
    out_refs[PIECES][...] = mass_ref[...].astype(jnp.bfloat16)


def split(state, mass):
    piece = pltpu.VMEM(state.shape[1:], jnp.bfloat16)
    return pl.pallas_call(
        split_kernel,
        out_shape=[piece] * PIECES + [pltpu.VMEM(mass.shape, jnp.bfloat16)],
        in_specs=[vmem()] * 2,
        out_specs=[vmem()] * (PIECES + 1),
        compiler_params=room(8),
        name="split",
    )(state, mass)


def pack_kernel(*refs):
    for i in range(PIECES):
        refs[PIECES][i] = refs[i][...]


def pack(pieces):
    return pl.pallas_call(
        pack_kernel,
        out_shape=pltpu.VMEM((PIECES, *pieces[0].shape), jnp.bfloat16),
        in_specs=[vmem()] * PIECES,
        out_specs=vmem(),
        compiler_params=room(4),
        name="pack",
    )(*pieces)


def project_kernel(mixed_ref, own_ref, other_ref, out_ref, weight_ref, wide_ref, sems):
    core = lax.axis_index("c")
    batch, heads, tokens, size = mixed_ref.shape
    blocks = out_ref.shape[1] // COLUMNS

    def moves(n):
        columns = pl.ds(n * COLUMNS, COLUMNS)
        return [
            pltpu.make_async_copy(
                source.at[:, :, columns], weight_ref.at[:, place, :, columns], sems.at[i, n]
            )
            for i, (source, place) in enumerate(((own_ref, core), (other_ref, 1 - core)))
        ]

    for n in range(blocks):
        for move in moves(n):
            move.start()
    for b in range(batch):
        for h in range(heads):
            rows = slice(b * tokens, (b + 1) * tokens)
            wide_ref[rows, h * size : (h + 1) * size] = mixed_ref[b, h]
    for n in range(blocks):
        for move in moves(n):
            move.wait()
        columns = slice(n * COLUMNS, (n + 1) * COLUMNS)
        block = weight_ref[:, :, :, columns].reshape(-1, COLUMNS)
        out_ref[:, columns] = jnp.dot(
            wide_ref[...], block, preferred_element_type=jnp.float32
        ).astype(out_ref.dtype)


def project(mixed, own, other):
    chips, rows, width = own.shape
    batch, heads, tokens, size = mixed.shape
    return pl.pallas_call(
        project_kernel,
        out_shape=jax.ShapeDtypeStruct((batch * tokens, width), jnp.bfloat16),
        in_specs=[vmem(), pl.BlockSpec(memory_space=pl.ANY), pl.BlockSpec(memory_space=pl.ANY)],
        out_specs=vmem(),
        scratch_shapes=[
            pltpu.VMEM((chips, 2, rows, width), jnp.bfloat16),
            pltpu.VMEM((batch * tokens, heads * size), jnp.bfloat16),
            pltpu.SemaphoreType.DMA((2, width // COLUMNS)),
        ],
        cost_estimate=pl.CostEstimate(
            flops=2 * mixed.size * width, bytes_accessed=4 * own.size, transcendentals=0
        ),
        compiler_params=room(20),
        name="project",
    )(mixed, own, other)


def local(query_rows, key_rows, value_rows, gate_rows, out_weight):
    own = lax.all_to_all(copies_of(out_weight, 16), ("y", "x"), 0, 0, tiled=True)
    query_feature, key_feature = (feature_map(query_rows), feature_map(key_rows))
    count = query_rows.shape[1] * lax.axis_size("z")
    part_state = jnp.einsum(
        "bthd,bthe->bhde", key_feature, value_rows, preferred_element_type=jnp.float32
    )
    part_mass = jnp.sum(key_feature.astype(jnp.float32), axis=1)
    parts = split(
        (part_state / count).reshape(PIECES, -1, part_state.shape[-1]),
        (part_mass / count).reshape(-1, part_mass.shape[-1]),
    )
    *state, mass = lax.psum(parts, "z")
    state = pack(state).reshape(part_state.shape)
    mass = mass.reshape(part_mass.shape).astype(jnp.float32)
    own, mass = lax.optimization_barrier((own, mass))
    other = lax.ppermute(own, "c", [(0, 1), (1, 0)])
    mixed = finish_heads(read_state(query_feature, state, mass), gate_rows, count)
    return project(mixed, own, other).reshape(*query_rows.shape[:2], -1)


def solution(mesh):
    grid = Mesh(mesh.devices.reshape(4, 4, 2, 16), ("y", "x", "c", "z"))
    rows = P(("y", "x", "c"), "z", None, None)
    in_specs = (rows, rows, rows, rows, P(("y", "x", "c"), None))
    out_specs = P(("y", "x", "c"), "z", None)
    return jax.shard_map(local, mesh=grid, in_specs=in_specs, out_specs=out_specs, check_vma=False)
```

```python
import jax
import jax.numpy as jnp
from jax import lax
from jax.experimental import pallas as pl
from jax.experimental.pallas import tpu as pltpu
from jax.sharding import Mesh, PartitionSpec as P

HEADS = 16
COLUMNS = 512
HBM = pl.BlockSpec(memory_space=pltpu.HBM)
HERE = pl.BlockSpec(memory_space=pltpu.VMEM)


def room(mib):
    return pltpu.CompilerParams(vmem_limit_bytes=mib * 2**20)


def stay(*arrays):
    return [pltpu.with_memory_space_constraint(array, pltpu.HBM) for array in arrays]


def feature_map(wide):
    return (wide * wide + 0.1).astype(jnp.bfloat16)


def of_head(ref, batch, head, tokens):
    return ref[batch, pl.ds(head, tokens, stride=HEADS), :]


def piece_moves(states, masses, pieces, mass_ref, sems, out):
    half = states.shape[1] // 2
    ends = [(masses, mass_ref)]
    for i, piece in enumerate(pieces):
        ends.append((states.at[i // 2, pl.ds(i % 2 * half, half), :], piece))
    return [
        pltpu.make_async_copy(*(pair if out else pair[::-1]), sems.at[i])
        for i, pair in enumerate(ends)
    ]


def sums_kernel(count, key_ref, value_ref, weight_ref, *refs):
    pieces = refs[:64]
    mass_ref, copies_ref, keys, values, wide_keys, wide_values, block, states, masses = refs[64:73]
    sems, out_sems, piece_sem = refs[73:]
    batch, rows, size = key_ref.shape
    tokens = rows // HEADS
    fetch_block = pltpu.make_async_copy(weight_ref, block, sems.at[0, 2])
    fetch_block.start()
    fetches = [
        [
            pltpu.make_async_copy(source.at[b], target.at[b], sems.at[b, i])
            for i, (source, target) in enumerate(((key_ref, keys), (value_ref, values)))
        ]
        for b in range(batch)
    ]
    for pair in fetches:
        for fetch in pair:
            fetch.start()
    fetch_block.wait()
    copies = [
        pltpu.make_async_copy(block, copies_ref.at[i], out_sems.at[i])
        for i in range(copies_ref.shape[0])
    ]
    for copy in copies:
        copy.start()
    for b in range(batch):
        for fetch in fetches[b]:
            fetch.wait()
        wide_keys[b] = keys[b].astype(jnp.float32)
        wide_values[b] = values[b].astype(jnp.float32)
        for h in range(HEADS):
            features = feature_map(of_head(wide_keys, b, h, tokens))
            head_values = of_head(wide_values, b, h, tokens).astype(jnp.bfloat16)
            state = lax.dot_general(
                features, head_values, (((0,), (0,)), ((), ())), preferred_element_type=jnp.float32
            )
            pair = b * HEADS + h
            states[pair] = (state * (1.0 / count)).astype(jnp.bfloat16)
            mass = jnp.sum(features.astype(jnp.float32), axis=0, keepdims=True)
            masses[pair : pair + 1, :] = (mass * (1.0 / count)).astype(jnp.bfloat16)
    moves = piece_moves(states, masses, pieces, mass_ref, piece_sem, True)
    for move in moves:
        move.start()
    for move in copies + moves:
        move.wait()


def part_sums(count, keys, values, weight):
    batch, rows, size = keys.shape
    piece = pltpu.HBM((size // 2, size), jnp.bfloat16)
    wide = pltpu.VMEM(keys.shape, jnp.float32)
    return pl.pallas_call(
        lambda *refs: sums_kernel(count, *refs),
        out_shape=[piece] * (4 * HEADS)
        + [
            pltpu.HBM((batch * HEADS, size), jnp.bfloat16),
            pltpu.HBM((HEADS, *weight.shape), weight.dtype),
        ],
        in_specs=[HBM] * 3,
        out_specs=[HBM] * (4 * HEADS + 2),
        scratch_shapes=[
            pltpu.VMEM(keys.shape, keys.dtype),
            pltpu.VMEM(values.shape, values.dtype),
            wide,
            wide,
            pltpu.VMEM(weight.shape, weight.dtype),
            pltpu.VMEM((batch * HEADS, size, size), jnp.bfloat16),
            pltpu.VMEM((batch * HEADS, size), jnp.bfloat16),
            pltpu.SemaphoreType.DMA((batch, 3)),
            pltpu.SemaphoreType.DMA((HEADS,)),
            pltpu.SemaphoreType.DMA((4 * HEADS + 1,)),
        ],
        compiler_params=room(24),
        name="sums",
    )(*stay(keys, values, weight))


def read_kernel(count, query_ref, gate_ref, own_ref, mass_ref, *refs):
    pieces = refs[:64]
    total_ref, rest_ref, wide_queries, wide_gates, weight, halves, states, masses = refs[64:72]
    sem, piece_sem = refs[72:]
    batch, rows, size = query_ref.shape
    tokens = rows // HEADS
    moves = piece_moves(states, masses, pieces, mass_ref, piece_sem, False)
    for move in moves:
        move.start()
    fetch_weight = pltpu.make_async_copy(own_ref, weight, sem)
    fetch_weight.start()
    first = lax.broadcasted_iota(jnp.int32, (tokens, size), 1) < size // 2
    core = lax.axis_index("c")
    for b in range(batch):
        wide_queries[b] = query_ref[b].astype(jnp.float32)
        wide_gates[b] = gate_ref[b].astype(jnp.float32)
        if b == 0:
            for move in moves:
                move.wait()
        mixed = []
        for h in range(HEADS):
            pair = b * HEADS + h
            features = feature_map(of_head(wide_queries, b, h, tokens))
            mass = jnp.broadcast_to(
                masses[pair : pair + 1, :].astype(jnp.float32), (size, size)
            ).astype(jnp.bfloat16)
            top = jnp.dot(features, states[pair], preferred_element_type=jnp.float32)
            bottom = lax.dot_general(
                features, mass, (((1,), (1,)), ((), ())), preferred_element_type=jnp.float32
            )
            gate = 1.0 + jnp.exp(-of_head(wide_gates, b, h, tokens))
            mixed.append(top * count**0.5 / ((bottom + 0.001) * gate))
            if h % 2:
                even, odd = mixed
                mixed = []
                place = (slice(b * tokens, (b + 1) * tokens), slice(h // 2 * size, (h // 2 + 1) * size))
                turned = pltpu.roll(odd, size // 2, 1)
                halves[0, *place] = jnp.where(first, even, turned).astype(jnp.bfloat16)
                turned = pltpu.roll(even, size // 2, 1)
                halves[1, *place] = jnp.where(first, turned, odd).astype(jnp.bfloat16)
    rest_ref[...] = halves[1 - core]
    fetch_weight.wait()
    for n in range(total_ref.shape[1] // COLUMNS):
        columns = slice(n * COLUMNS, (n + 1) * COLUMNS)
        total_ref[:, columns] = jnp.dot(
            halves[core],
            weight[:, :, columns].reshape(-1, COLUMNS),
            preferred_element_type=jnp.float32,
        )


def read(count, queries, gates, own, mass, pieces):
    batch, rows, size = queries.shape
    tokens, width = batch * rows // HEADS, own.shape[2]
    half = HEADS * size // 2
    wide = pltpu.VMEM(queries.shape, jnp.float32)
    return pl.pallas_call(
        lambda *refs: read_kernel(count, *refs),
        out_shape=[
            pltpu.VMEM((tokens, width), jnp.float32),
            pltpu.VMEM((tokens, half), jnp.bfloat16),
        ],
        in_specs=[HERE, HERE] + [HBM] * 66,
        out_specs=[HERE] * 2,
        scratch_shapes=[
            wide,
            wide,
            pltpu.VMEM(own.shape, own.dtype),
            pltpu.VMEM((2, tokens, half), jnp.bfloat16),
            pltpu.VMEM((batch * HEADS, size, size), jnp.bfloat16),
            pltpu.VMEM((batch * HEADS, size), jnp.bfloat16),
            pltpu.SemaphoreType.DMA,
            pltpu.SemaphoreType.DMA((4 * HEADS + 1,)),
        ],
        compiler_params=room(32),
        cost_estimate=pl.CostEstimate(
            flops=2 * tokens * half * width, bytes_accessed=16 * 2**20, transcendentals=0
        ),
        name="read",
    )(queries, gates, *stay(own, mass, *pieces))


def finish_kernel(total_ref, rest_ref, other_ref, out_ref):
    for n in range(out_ref.shape[1] // COLUMNS):
        columns = slice(n * COLUMNS, (n + 1) * COLUMNS)
        part = jnp.dot(
            rest_ref[...],
            other_ref[:, :, columns].reshape(-1, COLUMNS),
            preferred_element_type=jnp.float32,
        )
        out_ref[:, columns] = (total_ref[:, columns] + part).astype(out_ref.dtype)


def finish(total, rest, other):
    return pl.pallas_call(
        finish_kernel,
        out_shape=jax.ShapeDtypeStruct(total.shape, jnp.bfloat16),
        in_specs=[HERE] * 3,
        out_specs=HERE,
        compiler_params=room(16),
        cost_estimate=pl.CostEstimate(
            flops=2 * rest.size * total.shape[1], bytes_accessed=8 * 2**20, transcendentals=0
        ),
        name="finish",
    )(total, rest, other)


def local(query_rows, key_rows, value_rows, gate_rows, out_weight):
    batch, tokens, heads, size = query_rows.shape
    count = tokens * lax.axis_size("z")
    queries, keys, values, gates = (
        rows.reshape(batch, tokens * heads, size)
        for rows in (query_rows, key_rows, value_rows, gate_rows)
    )
    *pieces, mass, copies = part_sums(count, keys, values, out_weight)
    own = lax.all_to_all(copies, ("y", "x"), 0, 0, tiled=True)
    *pieces, mass = lax.psum([*pieces, mass], "z")
    own, mass = lax.optimization_barrier((own, mass))
    other = lax.ppermute(own, "c", [(0, 1), (1, 0)])
    total, rest = read(count, queries, gates, own, mass, pieces)
    return finish(total, rest, other).reshape(batch, tokens, heads * size)


def solution(mesh):
    grid = Mesh(mesh.devices.reshape(4, 4, 2, 16), ("y", "x", "c", "z"))
    rows = P(("y", "x", "c"), "z", None, None)
    in_specs = (rows, rows, rows, rows, P(("y", "x", "c"), None))
    out_specs = P(("y", "x", "c"), "z", None)
    return jax.shard_map(local, mesh=grid, in_specs=in_specs, out_specs=out_specs, check_vma=False)
```

```python
import jax
import jax.numpy as jnp
from jax import lax
from jax.experimental import pallas as pl
from jax.experimental.pallas import tpu as pltpu
from jax.sharding import Mesh, PartitionSpec as P

HEADS = 16
COLUMNS = 512
HBM = pl.BlockSpec(memory_space=pltpu.HBM)
HERE = pl.BlockSpec(memory_space=pltpu.VMEM)


def room(mib):
    return pltpu.CompilerParams(vmem_limit_bytes=mib * 2**20)


def stay(*arrays):
    return [pltpu.with_memory_space_constraint(array, pltpu.HBM) for array in arrays]


def feature_map(wide):
    return (wide * wide + 0.1).astype(jnp.bfloat16)


def by_head(rows, tokens):
    wide = rows.astype(jnp.float32).reshape(tokens, HEADS, rows.shape[-1])
    return jnp.swapaxes(wide, 0, 1)


def piece_moves(states, masses, pieces, mass_ref, sems, out):
    half = states.shape[1] // 2
    ends = [(masses, mass_ref)]
    for i, piece in enumerate(pieces):
        ends.append((states.at[i // 2, pl.ds(i % 2 * half, half), :], piece))
    return [
        pltpu.make_async_copy(*(pair if out else pair[::-1]), sems.at[i])
        for i, pair in enumerate(ends)
    ]


def sums_kernel(count, key_ref, value_ref, weight_ref, *refs):
    pieces = refs[:64]
    mass_ref, copies_ref, keys, values, block, states, masses = refs[64:71]
    sems, out_sems, piece_sem = refs[71:]
    batch, rows, size = key_ref.shape
    tokens = rows // HEADS
    fetch_block = pltpu.make_async_copy(weight_ref, block, sems.at[0, 2])
    fetches = [
        [
            pltpu.make_async_copy(source.at[b], target.at[b], sems.at[b, i])
            for i, (source, target) in enumerate(((key_ref, keys), (value_ref, values)))
        ]
        for b in range(batch)
    ]
    for fetch in (*fetches[0], fetch_block, *fetches[1]):
        fetch.start()
    copies = [
        pltpu.make_async_copy(block, copies_ref.at[i], out_sems.at[i])
        for i in range(copies_ref.shape[0])
    ]
    moves = piece_moves(states, masses, pieces, mass_ref, piece_sem, True)
    for b in range(batch):
        for fetch in fetches[b]:
            fetch.wait()
        if b == 0:
            fetch_block.wait()
            for copy in copies:
                copy.start()
        wide_keys = by_head(keys[b], tokens)
        wide_values = by_head(values[b], tokens)
        for h in range(HEADS):
            features = feature_map(wide_keys[h])
            head_values = wide_values[h].astype(jnp.bfloat16)
            state = lax.dot_general(
                features, head_values, (((0,), (0,)), ((), ())), preferred_element_type=jnp.float32
            )
            pair = b * HEADS + h
            states[pair] = (state * (1.0 / count)).astype(jnp.bfloat16)
            mass = jnp.sum(features.astype(jnp.float32), axis=0, keepdims=True)
            masses[pair : pair + 1, :] = (mass * (1.0 / count)).astype(jnp.bfloat16)
        for move in moves[1 + 2 * HEADS * b : 1 + 2 * HEADS * (b + 1)]:
            move.start()
    moves[0].start()
    for move in copies + moves:
        move.wait()


def part_sums(count, keys, values, weight):
    batch, rows, size = keys.shape
    piece = pltpu.HBM((size // 2, size), jnp.bfloat16)
    return pl.pallas_call(
        lambda *refs: sums_kernel(count, *refs),
        out_shape=[piece] * (4 * HEADS)
        + [
            pltpu.HBM((batch * HEADS, size), jnp.bfloat16),
            pltpu.HBM((HEADS, *weight.shape), weight.dtype),
        ],
        in_specs=[HBM] * 3,
        out_specs=[HBM] * (4 * HEADS + 2),
        scratch_shapes=[
            pltpu.VMEM(keys.shape, keys.dtype),
            pltpu.VMEM(values.shape, values.dtype),
            pltpu.VMEM(weight.shape, weight.dtype),
            pltpu.VMEM((batch * HEADS, size, size), jnp.bfloat16),
            pltpu.VMEM((batch * HEADS, size), jnp.bfloat16),
            pltpu.SemaphoreType.DMA((batch, 3)),
            pltpu.SemaphoreType.DMA((HEADS,)),
            pltpu.SemaphoreType.DMA((4 * HEADS + 1,)),
        ],
        compiler_params=room(24),
        name="sums",
    )(*stay(keys, values, weight))


def read_kernel(count, query_ref, gate_ref, own_ref, mass_ref, *refs):
    pieces = refs[:64]
    total_ref, rest_ref, weight, halves, states, masses = refs[64:70]
    sem, piece_sem = refs[70:]
    batch, rows, size = query_ref.shape
    tokens = rows // HEADS
    moves = piece_moves(states, masses, pieces, mass_ref, piece_sem, False)
    for move in moves:
        move.start()
    fetch_weight = pltpu.make_async_copy(own_ref, weight, sem)
    fetch_weight.start()
    first = lax.broadcasted_iota(jnp.int32, (tokens, size), 1) < size // 2
    core = lax.axis_index("c")
    for b in range(batch):
        wide_queries = by_head(query_ref[b], tokens)
        wide_gates = by_head(gate_ref[b], tokens)
        if b == 0:
            for move in moves:
                move.wait()
        mixed = []
        for h in range(HEADS):
            pair = b * HEADS + h
            features = feature_map(wide_queries[h])
            mass = jnp.broadcast_to(
                masses[pair : pair + 1, :].astype(jnp.float32), (size, size)
            ).astype(jnp.bfloat16)
            top = jnp.dot(features, states[pair], preferred_element_type=jnp.float32)
            bottom = lax.dot_general(
                features, mass, (((1,), (1,)), ((), ())), preferred_element_type=jnp.float32
            )
            gate = 1.0 + jnp.exp(-wide_gates[h])
            mixed.append(top * count**0.5 / ((bottom + 0.001) * gate))
            if h % 2:
                even, odd = mixed
                mixed = []
                place = (slice(b * tokens, (b + 1) * tokens), slice(h // 2 * size, (h // 2 + 1) * size))
                turned = pltpu.roll(odd, size // 2, 1)
                halves[0, *place] = jnp.where(first, even, turned).astype(jnp.bfloat16)
                turned = pltpu.roll(even, size // 2, 1)
                halves[1, *place] = jnp.where(first, turned, odd).astype(jnp.bfloat16)
    rest_ref[...] = halves[1 - core]
    fetch_weight.wait()
    for n in range(total_ref.shape[1] // COLUMNS):
        columns = slice(n * COLUMNS, (n + 1) * COLUMNS)
        total_ref[:, columns] = jnp.dot(
            halves[core],
            weight[:, :, columns].reshape(-1, COLUMNS),
            preferred_element_type=jnp.float32,
        )


def read(count, queries, gates, own, mass, pieces):
    batch, rows, size = queries.shape
    tokens, width = batch * rows // HEADS, own.shape[2]
    half = HEADS * size // 2
    return pl.pallas_call(
        lambda *refs: read_kernel(count, *refs),
        out_shape=[
            pltpu.VMEM((tokens, width), jnp.float32),
            pltpu.VMEM((tokens, half), jnp.bfloat16),
        ],
        in_specs=[HERE, HERE] + [HBM] * 66,
        out_specs=[HERE] * 2,
        scratch_shapes=[
            pltpu.VMEM(own.shape, own.dtype),
            pltpu.VMEM((2, tokens, half), jnp.bfloat16),
            pltpu.VMEM((batch * HEADS, size, size), jnp.bfloat16),
            pltpu.VMEM((batch * HEADS, size), jnp.bfloat16),
            pltpu.SemaphoreType.DMA,
            pltpu.SemaphoreType.DMA((4 * HEADS + 1,)),
        ],
        compiler_params=room(32),
        cost_estimate=pl.CostEstimate(
            flops=2 * tokens * half * width, bytes_accessed=16 * 2**20, transcendentals=0
        ),
        name="read",
    )(queries, gates, *stay(own, mass, *pieces))


def finish_kernel(total_ref, rest_ref, other_ref, out_ref, result, sems):
    moves = []
    for n in range(out_ref.shape[1] // COLUMNS):
        columns = slice(n * COLUMNS, (n + 1) * COLUMNS)
        part = jnp.dot(
            rest_ref[...],
            other_ref[:, :, columns].reshape(-1, COLUMNS),
            preferred_element_type=jnp.float32,
        )
        result[:, columns] = (total_ref[:, columns] + part).astype(out_ref.dtype)
        move = pltpu.make_async_copy(result.at[:, columns], out_ref.at[:, columns], sems.at[n])
        move.start()
        moves.append(move)
    for move in moves:
        move.wait()


def finish(total, rest, other):
    return pl.pallas_call(
        finish_kernel,
        out_shape=jax.ShapeDtypeStruct(total.shape, jnp.bfloat16),
        in_specs=[HERE] * 3,
        out_specs=HBM,
        scratch_shapes=[
            pltpu.VMEM(total.shape, jnp.bfloat16),
            pltpu.SemaphoreType.DMA((total.shape[1] // COLUMNS,)),
        ],
        compiler_params=room(16),
        cost_estimate=pl.CostEstimate(
            flops=2 * rest.size * total.shape[1], bytes_accessed=8 * 2**20, transcendentals=0
        ),
        name="finish",
    )(total, rest, other)


def local(query_rows, key_rows, value_rows, gate_rows, out_weight):
    batch, tokens, heads, size = query_rows.shape
    count = tokens * lax.axis_size("z")
    queries, keys, values, gates = (
        rows.reshape(batch, tokens * heads, size)
        for rows in (query_rows, key_rows, value_rows, gate_rows)
    )
    *pieces, mass, copies = part_sums(count, keys, values, out_weight)
    own = lax.all_to_all(copies, ("y", "x"), 0, 0, tiled=True)
    *pieces, mass = lax.psum([*pieces, mass], "z")
    own, mass = lax.optimization_barrier((own, mass))
    other = lax.ppermute(own, "c", [(0, 1), (1, 0)])
    total, rest = read(count, queries, gates, own, mass, pieces)
    return finish(total, rest, other).reshape(batch, tokens, heads * size)


def solution(mesh):
    grid = Mesh(mesh.devices.reshape(4, 4, 2, 16), ("y", "x", "c", "z"))
    rows = P(("y", "x", "c"), "z", None, None)
    in_specs = (rows, rows, rows, rows, P(("y", "x", "c"), None))
    out_specs = P(("y", "x", "c"), "z", None)
    return jax.shard_map(local, mesh=grid, in_specs=in_specs, out_specs=out_specs, check_vma=False)
```

```python
import jax
import jax.numpy as jnp
from jax import lax
from jax.experimental import pallas as pl
from jax.experimental.pallas import tpu as pltpu
from jax.sharding import Mesh, PartitionSpec as P

HEADS = 16
COLUMNS = 512
HBM = pl.BlockSpec(memory_space=pltpu.HBM)
HERE = pl.BlockSpec(memory_space=pltpu.VMEM)


def room(mib):
    return pltpu.CompilerParams(vmem_limit_bytes=mib * 2**20)


def stay(*arrays):
    return [pltpu.with_memory_space_constraint(array, pltpu.HBM) for array in arrays]


def feature_map(wide):
    return (wide * wide + 0.1).astype(jnp.bfloat16)


def by_head(rows, tokens):
    wide = rows.astype(jnp.float32).reshape(tokens, HEADS, rows.shape[-1])
    return jnp.swapaxes(wide, 0, 1)


def piece_moves(states, masses, pieces, mass_ref, sems, out):
    half = states.shape[1] // 2
    ends = [(masses, mass_ref)]
    for i, piece in enumerate(pieces):
        ends.append((states.at[i // 2, pl.ds(i % 2 * half, half), :], piece))
    return [
        pltpu.make_async_copy(*(pair if out else pair[::-1]), sems.at[i])
        for i, pair in enumerate(ends)
    ]


def sums_kernel(count, key_ref, value_ref, weight_ref, *refs):
    pieces = refs[:64]
    mass_ref, copies_ref, keys, values, block, states, masses = refs[64:71]
    sems, out_sems, piece_sem = refs[71:]
    batch, rows, size = key_ref.shape
    tokens = rows // HEADS
    fetch_block = pltpu.make_async_copy(weight_ref, block, sems.at[0, 2])
    fetches = [
        [
            pltpu.make_async_copy(source.at[b], target.at[b], sems.at[b, i])
            for i, (source, target) in enumerate(((key_ref, keys), (value_ref, values)))
        ]
        for b in range(batch)
    ]
    for fetch in (fetch_block, *fetches[0], *fetches[1]):
        fetch.start()
    copies = [
        pltpu.make_async_copy(block, copies_ref.at[i], out_sems.at[i])
        for i in range(copies_ref.shape[0])
    ]
    fetch_block.wait()
    for copy in copies:
        copy.start()
    moves = piece_moves(states, masses, pieces, mass_ref, piece_sem, True)
    for b in range(batch):
        for fetch in fetches[b]:
            fetch.wait()
        wide_keys = by_head(keys[b], tokens)
        wide_values = by_head(values[b], tokens)
        for h in range(HEADS):
            features = feature_map(wide_keys[h])
            head_values = wide_values[h].astype(jnp.bfloat16)
            state = lax.dot_general(
                features, head_values, (((0,), (0,)), ((), ())), preferred_element_type=jnp.float32
            )
            pair = b * HEADS + h
            states[pair] = (state * (1.0 / count)).astype(jnp.bfloat16)
            mass = jnp.sum(features.astype(jnp.float32), axis=0, keepdims=True)
            masses[pair : pair + 1, :] = (mass * (1.0 / count)).astype(jnp.bfloat16)
            if h % 4 == 3:
                for move in moves[2 * pair - 5 : 2 * pair + 3]:
                    move.start()
    moves[0].start()
    for move in copies + moves:
        move.wait()


def part_sums(count, keys, values, weight):
    batch, rows, size = keys.shape
    piece = pltpu.HBM((size // 2, size), jnp.bfloat16)
    return pl.pallas_call(
        lambda *refs: sums_kernel(count, *refs),
        out_shape=[piece] * (4 * HEADS)
        + [
            pltpu.HBM((batch * HEADS, size), jnp.bfloat16),
            pltpu.HBM((HEADS, *weight.shape), weight.dtype),
        ],
        in_specs=[HBM] * 3,
        out_specs=[HBM] * (4 * HEADS + 2),
        scratch_shapes=[
            pltpu.VMEM(keys.shape, keys.dtype),
            pltpu.VMEM(values.shape, values.dtype),
            pltpu.VMEM(weight.shape, weight.dtype),
            pltpu.VMEM((batch * HEADS, size, size), jnp.bfloat16),
            pltpu.VMEM((batch * HEADS, size), jnp.bfloat16),
            pltpu.SemaphoreType.DMA((batch, 3)),
            pltpu.SemaphoreType.DMA((HEADS,)),
            pltpu.SemaphoreType.DMA((4 * HEADS + 1,)),
        ],
        compiler_params=room(24),
        name="sums",
    )(*stay(keys, values, weight))


def read_kernel(count, query_ref, gate_ref, own_ref, mass_ref, *refs):
    pieces = refs[:64]
    total_ref, rest_ref, weight, halves, states, masses = refs[64:70]
    sem, piece_sem = refs[70:]
    batch, rows, size = query_ref.shape
    tokens = rows // HEADS
    moves = piece_moves(states, masses, pieces, mass_ref, piece_sem, False)
    for move in moves:
        move.start()
    fetch_weight = pltpu.make_async_copy(own_ref, weight, sem)
    fetch_weight.start()
    first = lax.broadcasted_iota(jnp.int32, (tokens, size), 1) < size // 2
    core = lax.axis_index("c")
    for b in range(batch):
        wide_queries = by_head(query_ref[b], tokens)
        wide_gates = by_head(gate_ref[b], tokens)
        if b == 0:
            for move in moves:
                move.wait()
        mixed = []
        for h in range(HEADS):
            pair = b * HEADS + h
            features = feature_map(wide_queries[h])
            mass = jnp.broadcast_to(
                masses[pair : pair + 1, :].astype(jnp.float32), (size, size)
            ).astype(jnp.bfloat16)
            top = jnp.dot(features, states[pair], preferred_element_type=jnp.float32)
            bottom = lax.dot_general(
                features, mass, (((1,), (1,)), ((), ())), preferred_element_type=jnp.float32
            )
            gate = 1.0 + jnp.exp(-wide_gates[h])
            mixed.append(top * count**0.5 / ((bottom + 0.001) * gate))
            if h % 2:
                even, odd = mixed
                mixed = []
                place = (slice(b * tokens, (b + 1) * tokens), slice(h // 2 * size, (h // 2 + 1) * size))
                turned = pltpu.roll(odd, size // 2, 1)
                halves[0, *place] = jnp.where(first, even, turned).astype(jnp.bfloat16)
                turned = pltpu.roll(even, size // 2, 1)
                halves[1, *place] = jnp.where(first, turned, odd).astype(jnp.bfloat16)
    rest_ref[...] = halves[1 - core]
    fetch_weight.wait()
    for n in range(total_ref.shape[1] // COLUMNS):
        columns = slice(n * COLUMNS, (n + 1) * COLUMNS)
        total_ref[:, columns] = jnp.dot(
            halves[core],
            weight[:, :, columns].reshape(-1, COLUMNS),
            preferred_element_type=jnp.float32,
        )


def read(count, queries, gates, own, mass, pieces):
    batch, rows, size = queries.shape
    tokens, width = batch * rows // HEADS, own.shape[2]
    half = HEADS * size // 2
    return pl.pallas_call(
        lambda *refs: read_kernel(count, *refs),
        out_shape=[
            pltpu.VMEM((tokens, width), jnp.float32),
            pltpu.VMEM((tokens, half), jnp.bfloat16),
        ],
        in_specs=[HERE, HERE] + [HBM] * 66,
        out_specs=[HERE] * 2,
        scratch_shapes=[
            pltpu.VMEM(own.shape, own.dtype),
            pltpu.VMEM((2, tokens, half), jnp.bfloat16),
            pltpu.VMEM((batch * HEADS, size, size), jnp.bfloat16),
            pltpu.VMEM((batch * HEADS, size), jnp.bfloat16),
            pltpu.SemaphoreType.DMA,
            pltpu.SemaphoreType.DMA((4 * HEADS + 1,)),
        ],
        compiler_params=room(32),
        cost_estimate=pl.CostEstimate(
            flops=2 * tokens * half * width, bytes_accessed=16 * 2**20, transcendentals=0
        ),
        name="read",
    )(queries, gates, *stay(own, mass, *pieces))


def finish_kernel(total_ref, rest_ref, other_ref, out_ref, result, sems):
    moves = []
    for n in range(out_ref.shape[1] // COLUMNS):
        columns = slice(n * COLUMNS, (n + 1) * COLUMNS)
        part = jnp.dot(
            rest_ref[...],
            other_ref[:, :, columns].reshape(-1, COLUMNS),
            preferred_element_type=jnp.float32,
        )
        result[:, columns] = (total_ref[:, columns] + part).astype(out_ref.dtype)
        move = pltpu.make_async_copy(result.at[:, columns], out_ref.at[:, columns], sems.at[n])
        move.start()
        moves.append(move)
    for move in moves:
        move.wait()


def finish(total, rest, other):
    return pl.pallas_call(
        finish_kernel,
        out_shape=jax.ShapeDtypeStruct(total.shape, jnp.bfloat16),
        in_specs=[HERE] * 3,
        out_specs=HBM,
        scratch_shapes=[
            pltpu.VMEM(total.shape, jnp.bfloat16),
            pltpu.SemaphoreType.DMA((total.shape[1] // COLUMNS,)),
        ],
        compiler_params=room(16),
        cost_estimate=pl.CostEstimate(
            flops=2 * rest.size * total.shape[1], bytes_accessed=8 * 2**20, transcendentals=0
        ),
        name="finish",
    )(total, rest, other)


def local(query_rows, key_rows, value_rows, gate_rows, out_weight):
    batch, tokens, heads, size = query_rows.shape
    count = tokens * lax.axis_size("z")
    queries, keys, values, gates = (
        rows.reshape(batch, tokens * heads, size)
        for rows in (query_rows, key_rows, value_rows, gate_rows)
    )
    *pieces, mass, copies = part_sums(count, keys, values, out_weight)
    own = lax.all_to_all(copies, ("y", "x"), 0, 0, tiled=True)
    *pieces, mass = lax.psum([*pieces, mass], "z")
    own, mass = lax.optimization_barrier((own, mass))
    other = lax.ppermute(own, "c", [(0, 1), (1, 0)])
    total, rest = read(count, queries, gates, own, mass, pieces)
    return finish(total, rest, other).reshape(batch, tokens, heads * size)


def solution(mesh):
    grid = Mesh(mesh.devices.reshape(4, 4, 2, 16), ("y", "x", "c", "z"))
    rows = P(("y", "x", "c"), "z", None, None)
    in_specs = (rows, rows, rows, rows, P(("y", "x", "c"), None))
    out_specs = P(("y", "x", "c"), "z", None)
    return jax.shard_map(local, mesh=grid, in_specs=in_specs, out_specs=out_specs, check_vma=False)
```

```python
import jax
import jax.numpy as jnp
from jax import lax
from jax.experimental import pallas as pl
from jax.experimental.pallas import tpu as pltpu
from jax.sharding import Mesh, PartitionSpec as P

HEADS = 16
COLUMNS = 512
LAST_COLUMNS = (768, 512, 512, 256)
HBM = pl.BlockSpec(memory_space=pltpu.HBM)
HERE = pl.BlockSpec(memory_space=pltpu.VMEM)


def room(mib):
    return pltpu.CompilerParams(vmem_limit_bytes=mib * 2**20)


def stay(*arrays):
    return [pltpu.with_memory_space_constraint(array, pltpu.HBM) for array in arrays]


def feature_map(wide):
    return (wide * wide + 0.1).astype(jnp.bfloat16)


def by_head(rows, tokens):
    wide = rows.astype(jnp.float32).reshape(tokens, HEADS, rows.shape[-1])
    return jnp.swapaxes(wide, 0, 1)


def piece_moves(states, masses, pieces, mass_ref, sems, out):
    half = states.shape[1] // 2
    ends = [(masses, mass_ref)]
    for i, piece in enumerate(pieces):
        ends.append((states.at[i // 2, pl.ds(i % 2 * half, half), :], piece))
    return [
        pltpu.make_async_copy(*(pair if out else pair[::-1]), sems.at[i])
        for i, pair in enumerate(ends)
    ]


def sums_kernel(count, key_ref, value_ref, weight_ref, *refs):
    pieces = refs[:64]
    mass_ref, copies_ref, keys, values, block, states, masses = refs[64:71]
    sems, out_sems, piece_sem = refs[71:]
    batch, rows, size = key_ref.shape
    tokens = rows // HEADS
    fetch_block = pltpu.make_async_copy(weight_ref, block, sems.at[0, 2])
    fetches = [
        [
            pltpu.make_async_copy(source.at[b], target.at[b], sems.at[b, i])
            for i, (source, target) in enumerate(((key_ref, keys), (value_ref, values)))
        ]
        for b in range(batch)
    ]
    for fetch in (fetch_block, *fetches[0], *fetches[1]):
        fetch.start()
    copies = [
        pltpu.make_async_copy(block, copies_ref.at[i], out_sems.at[i])
        for i in range(copies_ref.shape[0])
    ]
    fetch_block.wait()
    for copy in copies:
        copy.start()
    moves = piece_moves(states, masses, pieces, mass_ref, piece_sem, True)
    for b in range(batch):
        for fetch in fetches[b]:
            fetch.wait()
        wide_keys = by_head(keys[b], tokens)
        wide_values = by_head(values[b], tokens)
        for h in range(HEADS):
            features = feature_map(wide_keys[h])
            head_values = wide_values[h].astype(jnp.bfloat16)
            state = lax.dot_general(
                features, head_values, (((0,), (0,)), ((), ())), preferred_element_type=jnp.float32
            )
            pair = b * HEADS + h
            states[pair] = (state * (1.0 / count)).astype(jnp.bfloat16)
            mass = jnp.sum(features.astype(jnp.float32), axis=0, keepdims=True)
            masses[pair : pair + 1, :] = (mass * (1.0 / count)).astype(jnp.bfloat16)
            if h % 4 == 3:
                for move in moves[2 * pair - 5 : 2 * pair + 3]:
                    move.start()
    moves[0].start()
    for move in copies + moves:
        move.wait()


def part_sums(count, keys, values, weight):
    batch, rows, size = keys.shape
    piece = pltpu.HBM((size // 2, size), jnp.bfloat16)
    return pl.pallas_call(
        lambda *refs: sums_kernel(count, *refs),
        out_shape=[piece] * (4 * HEADS)
        + [
            pltpu.HBM((batch * HEADS, size), jnp.bfloat16),
            pltpu.HBM((HEADS, *weight.shape), weight.dtype),
        ],
        in_specs=[HBM] * 3,
        out_specs=[HBM] * (4 * HEADS + 2),
        scratch_shapes=[
            pltpu.VMEM(keys.shape, keys.dtype),
            pltpu.VMEM(values.shape, values.dtype),
            pltpu.VMEM(weight.shape, weight.dtype),
            pltpu.VMEM((batch * HEADS, size, size), jnp.bfloat16),
            pltpu.VMEM((batch * HEADS, size), jnp.bfloat16),
            pltpu.SemaphoreType.DMA((batch, 3)),
            pltpu.SemaphoreType.DMA((HEADS,)),
            pltpu.SemaphoreType.DMA((4 * HEADS + 1,)),
        ],
        compiler_params=room(24),
        name="sums",
    )(*stay(keys, values, weight))


def read_kernel(count, query_ref, gate_ref, own_ref, mass_ref, *refs):
    pieces = refs[:64]
    total_ref, rest_ref, weight, halves, states, masses = refs[64:70]
    sem, piece_sem = refs[70:]
    batch, rows, size = query_ref.shape
    tokens = rows // HEADS
    moves = piece_moves(states, masses, pieces, mass_ref, piece_sem, False)
    for move in moves:
        move.start()
    fetch_weight = pltpu.make_async_copy(own_ref, weight, sem)
    fetch_weight.start()
    first = lax.broadcasted_iota(jnp.int32, (tokens, size), 1) < size // 2
    core = lax.axis_index("c")
    for b in range(batch):
        wide_queries = by_head(query_ref[b], tokens)
        wide_gates = by_head(gate_ref[b], tokens)
        if b == 0:
            for move in moves:
                move.wait()
        mixed = []
        for h in range(HEADS):
            pair = b * HEADS + h
            features = feature_map(wide_queries[h])
            mass = jnp.broadcast_to(
                masses[pair : pair + 1, :].astype(jnp.float32), (size, size)
            ).astype(jnp.bfloat16)
            top = jnp.dot(features, states[pair], preferred_element_type=jnp.float32)
            bottom = lax.dot_general(
                features, mass, (((1,), (1,)), ((), ())), preferred_element_type=jnp.float32
            )
            gate = 1.0 + jnp.exp(-wide_gates[h])
            mixed.append(top * count**0.5 / ((bottom + 0.001) * gate))
            if h % 2:
                even, odd = mixed
                mixed = []
                place = (slice(b * tokens, (b + 1) * tokens), slice(h // 2 * size, (h // 2 + 1) * size))
                turned = pltpu.roll(odd, size // 2, 1)
                halves[0, *place] = jnp.where(first, even, turned).astype(jnp.bfloat16)
                turned = pltpu.roll(even, size // 2, 1)
                halves[1, *place] = jnp.where(first, turned, odd).astype(jnp.bfloat16)
    rest_ref[...] = halves[1 - core]
    fetch_weight.wait()
    for n in range(total_ref.shape[1] // COLUMNS):
        columns = slice(n * COLUMNS, (n + 1) * COLUMNS)
        total_ref[:, columns] = jnp.dot(
            halves[core],
            weight[:, :, columns].reshape(-1, COLUMNS),
            preferred_element_type=jnp.float32,
        )


def read(count, queries, gates, own, mass, pieces):
    batch, rows, size = queries.shape
    tokens, width = batch * rows // HEADS, own.shape[2]
    half = HEADS * size // 2
    return pl.pallas_call(
        lambda *refs: read_kernel(count, *refs),
        out_shape=[
            pltpu.VMEM((tokens, width), jnp.float32),
            pltpu.VMEM((tokens, half), jnp.bfloat16),
        ],
        in_specs=[HERE, HERE] + [HBM] * 66,
        out_specs=[HERE] * 2,
        scratch_shapes=[
            pltpu.VMEM(own.shape, own.dtype),
            pltpu.VMEM((2, tokens, half), jnp.bfloat16),
            pltpu.VMEM((batch * HEADS, size, size), jnp.bfloat16),
            pltpu.VMEM((batch * HEADS, size), jnp.bfloat16),
            pltpu.SemaphoreType.DMA,
            pltpu.SemaphoreType.DMA((4 * HEADS + 1,)),
        ],
        compiler_params=room(32),
        cost_estimate=pl.CostEstimate(
            flops=2 * tokens * half * width, bytes_accessed=16 * 2**20, transcendentals=0
        ),
        name="read",
    )(queries, gates, *stay(own, mass, *pieces))


def finish_kernel(total_ref, rest_ref, other_ref, out_ref, result, sems):
    moves = []
    start = 0
    for n, size in enumerate(LAST_COLUMNS):
        columns = slice(start, start + size)
        start += size
        part = jnp.dot(
            rest_ref[...],
            other_ref[:, :, columns].reshape(-1, size),
            preferred_element_type=jnp.float32,
        )
        result[:, columns] = (total_ref[:, columns] + part).astype(out_ref.dtype)
        move = pltpu.make_async_copy(result.at[:, columns], out_ref.at[:, columns], sems.at[n])
        move.start()
        moves.append(move)
    for move in moves:
        move.wait()


def finish(total, rest, other):
    return pl.pallas_call(
        finish_kernel,
        out_shape=jax.ShapeDtypeStruct(total.shape, jnp.bfloat16),
        in_specs=[HERE] * 3,
        out_specs=HBM,
        scratch_shapes=[
            pltpu.VMEM(total.shape, jnp.bfloat16),
            pltpu.SemaphoreType.DMA((len(LAST_COLUMNS),)),
        ],
        compiler_params=room(16),
        cost_estimate=pl.CostEstimate(
            flops=2 * rest.size * total.shape[1], bytes_accessed=8 * 2**20, transcendentals=0
        ),
        name="finish",
    )(total, rest, other)


def local(query_rows, key_rows, value_rows, gate_rows, out_weight):
    batch, tokens, heads, size = query_rows.shape
    count = tokens * lax.axis_size("z")
    queries, keys, values, gates = (
        rows.reshape(batch, tokens * heads, size)
        for rows in (query_rows, key_rows, value_rows, gate_rows)
    )
    *pieces, mass, copies = part_sums(count, keys, values, out_weight)
    own = lax.all_to_all(copies, ("y", "x"), 0, 0, tiled=True)
    *pieces, mass = lax.psum([*pieces, mass], "z")
    own, mass = lax.optimization_barrier((own, mass))
    other = lax.ppermute(own, "c", [(0, 1), (1, 0)])
    total, rest = read(count, queries, gates, own, mass, pieces)
    return finish(total, rest, other).reshape(batch, tokens, heads * size)


def solution(mesh):
    grid = Mesh(mesh.devices.reshape(4, 4, 2, 16), ("y", "x", "c", "z"))
    rows = P(("y", "x", "c"), "z", None, None)
    in_specs = (rows, rows, rows, rows, P(("y", "x", "c"), None))
    out_specs = P(("y", "x", "c"), "z", None)
    return jax.shard_map(local, mesh=grid, in_specs=in_specs, out_specs=out_specs, check_vma=False)
```
